32 devices in a mesh: member: 4 (over y, x), space: 8 (over z, core).
Axes of the slice: x: 2, y: 2, z: 4, core: 2. Of those that a mesh axis runs over, the one named last changes fastest.
Arguments:
- ensemble_prediction: bfloat16 [4, 300, 128, 128], P('member', None, 'space'), may hold values from -6 to 6
- observed_analysis: bfloat16 [300, 128, 128], P(None, 'space'), may hold values from -6 to 6
- validity_flags: int32 [2, 128, 128], P(None, 'space'), may hold values from 0 to 1, as said below
Outputs:
- point_score: float32 [300, 128, 128], P(None, 'space')
- channel_loss: float32 [300], replicated
The draws below stay inside these ranges and needn't reach their ends.
Inputs may be any that keep to these rules, and one draw needn't show every extreme that they name: `validity_flags`: 0 or 1 for each point and group; every point of latitude row 11 is valid in both groups.
All inputs are finite; a program needn't handle non-finite values.
Results may differ from the reference program's by a relative error of at most 0.0003.
Values may be sent and summed in bfloat16 or wider, within the bound.
A program may use at most 64 MiB of HBM per device.

```python
import jax
import jax.numpy as jnp

VARIABLE_NUMBER = 300
ATMOS = 180
GROUPS = 2
TILE_SITES = 128
LON = 720
TILE_NUMBER = 128
LAT = 22
ENSEMBLE_SIZE = 4


def draw_validity_flags(key, part):
    position = jnp.arange(TILE_NUMBER * TILE_SITES, dtype=jnp.int32).reshape(TILE_NUMBER, TILE_SITES)
    lat_row = position // LON
    atmos_thr = 300 + 650 * lat_row // LAT
    ocean_thr = 150 + 750 * lat_row // LAT
    thresholds = jnp.stack([atmos_thr, ocean_thr])
    rolled = jax.random.randint(jax.random.fold_in(key, 17), (GROUPS, TILE_NUMBER, TILE_SITES), 0, 1000)
    drawn = (rolled < thresholds).astype(jnp.int32)
    middle = (lat_row == LAT // 2)[None]
    return jnp.where(middle, 1, drawn).astype(jnp.int32)


def level_of(rng, dims, shards, least, top_value):
    def one(dim, parts):
        steps = jax.random.uniform(jax.random.fold_in(jax.random.fold_in(rng, 6), dim), (parts,), jnp.float32, least / len(shards), top_value / len(shards))
        return jnp.repeat(jnp.exp(steps), dims[dim] // parts).reshape((-1,) + (1,) * (len(dims) - dim - 1))

    level = one(*shards[0])
    for cut in shards[1:]:
        level = level * one(*cut)
    return level


def noise(stream_key, extent, deviation, bound, split=(), held_as=jnp.bfloat16):
    values = deviation * jax.random.normal(stream_key, extent, jnp.float32)
    if split:
        values = values * level_of(stream_key, extent, split, -0.22, 0.18)
    return jnp.clip(values, -bound, bound).astype(held_as)


def setup_inputs(seed: int = 0) -> dict:
    key_of = jax.random.split(jax.random.key(seed), 4)
    return {
        "ensemble_prediction": noise(key_of[0], (ENSEMBLE_SIZE, VARIABLE_NUMBER, TILE_NUMBER, TILE_SITES), 1.0, 6.0, ((0, 4), (2, 8))),
        "observed_analysis": noise(key_of[1], (VARIABLE_NUMBER, TILE_NUMBER, TILE_SITES), 1.0, 6.0, ((1, 8),)),
        "validity_flags": draw_validity_flags(jax.random.fold_in(key_of[3], 71), 0),
    }


def reference(ensemble_prediction, observed_analysis, validity_flags):
    realization_entries = ensemble_prediction.shape[0]
    position = jnp.arange(TILE_NUMBER * TILE_SITES, dtype=jnp.int32).reshape(TILE_NUMBER, TILE_SITES)
    inside = (position < LAT * LON).astype(jnp.float32)
    lat_row = (position // LON).astype(jnp.float32)
    cosine = jnp.cos(jnp.pi * ((lat_row + 0.5) / LAT - 0.5))
    valid = inside[None] * (validity_flags > 0).astype(jnp.float32)
    weight = cosine[None] * valid
    area_sum = jnp.sum(weight, axis=(1, 2))
    count = jnp.sum(valid, axis=(1, 2))
    is_ocean = jnp.arange(VARIABLE_NUMBER, dtype=jnp.int32) >= ATMOS
    weight_chan = jnp.where(is_ocean[:, None, None], weight[1][None], weight[0][None])
    observed_real_entries = observed_analysis.astype(jnp.float32)
    accuracy_component = jnp.zeros(observed_analysis.shape, jnp.float32)
    for leading_realization in range(realization_entries):
        accuracy_component = accuracy_component + jnp.abs(ensemble_prediction[leading_realization].astype(jnp.float32) - observed_real_entries)
    dispersion_component = jnp.zeros(observed_analysis.shape, jnp.float32)
    for leading_realization in range(realization_entries):
        for trailing_realization in range(leading_realization + 1, realization_entries):
            dispersion_component = dispersion_component + jnp.abs(ensemble_prediction[leading_realization].astype(jnp.float32) - ensemble_prediction[trailing_realization].astype(jnp.float32))
    dispersion_component = 2.0 * dispersion_component
    coeff = (1.0 - 0.05 / realization_entries) / (2.0 * realization_entries * (realization_entries - 1))
    crps = accuracy_component / realization_entries - coeff * dispersion_component
    scale_chan = jnp.where(is_ocean, count[1] / area_sum[1], count[0] / area_sum[0])
    count_chan = jnp.where(is_ocean, count[1], count[0])
    point_score = crps * weight_chan * scale_chan[:, None, None]
    channel_loss = jnp.sum(point_score, axis=(1, 2)) / count_chan
    return point_score, channel_loss
```

```python
import functools

import jax
import jax.numpy as jnp
from jax import lax
from jax.experimental import pallas as pl
from jax.experimental.pallas import tpu as pltpu
from jax.sharding import PartitionSpec as P

ATMOS = 180
LON = 720
ROWS = 360
MESH = pl.DeviceIdType.MESH

CODES = 1638.0
CENTRE = 16.0
SMALLEST = 2.0**-36
ABSENT = -32768
INV_LN2 = 1.4426950408889634


def encode(value):
    steps = (jnp.log(jnp.maximum(value, SMALLEST)) * INV_LN2 + CENTRE) * CODES
    code = jnp.floor(steps + 0.5).astype(jnp.int32)
    return jnp.where(value < SMALLEST, ABSENT, code).astype(jnp.int16)


def decode(code):
    code = code.astype(jnp.int32)
    value = jnp.exp2(code.astype(jnp.float32) * (1.0 / CODES) - CENTRE)
    return jnp.where(code == ABSENT, 0.0, value)


def pieces(share, parts):
    edges = [share * i // parts for i in range(parts + 1)]
    return [(a, b - a) for a, b in zip(edges[:-1], edges[1:])]


def kernel(
    members, spaces, share, parts,
    ens_ref, obs_ref, flags_ref,
    code_ref, weight_ref, loss_ref,
    own, target, arrived, totals, stats, sums, gathered,
    local_sem, send_a, recv_a, send_b, recv_b, send_c, recv_c,
    send_s, recv_s, send_t, recv_t, send_u, recv_u,
):
    me = lax.axis_index("member")
    here = lax.axis_index("space")
    x_peer = me + 1 - 2 * lax.rem(me, 2)
    y_peer = lax.rem(me + 2, 4)
    diagonal = 3 - me
    peers = (x_peer, y_peer, diagonal)
    cuts = pieces(share, parts)

    def remote(src, dst, send, recv, where):
        return pltpu.make_async_remote_copy(
            src_ref=src, dst_ref=dst, send_sem=send, recv_sem=recv,
            device_id=where, device_id_type=MESH,
        )

    mine = pltpu.make_async_copy(ens_ref.at[0, pl.ds(me * share, share)], own, local_sem.at[0])
    aim = pltpu.make_async_copy(obs_ref.at[pl.ds(me * share, share)], target, local_sem.at[1])
    mine.start()
    aim.start()

    barrier = pltpu.get_barrier_semaphore()
    for peer in peers:
        pl.semaphore_signal(barrier, inc=1, device_id={"member": peer}, device_id_type=MESH)

    def greet(i, carry):
        pl.semaphore_signal(
            barrier, inc=1, device_id={"space": lax.rem(here + i, spaces)}, device_id_type=MESH
        )
        return carry

    lax.fori_loop(1, spaces, greet, 0)
    pl.semaphore_wait(barrier, 3 + spaces - 1)

    def exchange(j, k):
        first, length = cuts[k]
        return remote(
            ens_ref.at[0, pl.ds(peers[j] * share + first, length)],
            arrived.at[j, pl.ds(first, length)],
            send_a.at[j, k], recv_a.at[j, k], {"member": peers[j]},
        )

    for k in range(parts):
        for j in (2, 0, 1):
            exchange(j, k).start()

    blocks, sites = flags_ref.shape[1], flags_ref.shape[2]
    lat_rows = min(ROWS, blocks * spaces * sites // LON)
    position = (
        here * (blocks * sites)
        + lax.broadcasted_iota(jnp.int32, (blocks, sites), 0) * sites
        + lax.broadcasted_iota(jnp.int32, (blocks, sites), 1)
    )
    inside = (position < lat_rows * LON).astype(jnp.float32)
    row = jnp.floor((position.astype(jnp.float32) + 0.5) * (1.0 / LON))
    cosine = jnp.cos(jnp.pi * ((row + 0.5) / lat_rows - 0.5))
    weights = []
    for g in range(2):
        valid = inside * (flags_ref[g] > 0).astype(jnp.float32)
        weight = cosine * valid
        weights.append(weight)
        weight_ref[g] = weight
        for r, part in ((g, weight), (2 + g, valid)):
            stats[here, pl.ds(r, 1)] = jnp.sum(part, axis=0, keepdims=True)

    def along_space(buffer, send, recv, i):
        return remote(
            buffer.at[here], buffer.at[here], send.at[i], recv.at[here],
            {"space": lax.rem(here + i, spaces)},
        )

    def from_space(buffer, send, recv, i):
        peer = lax.rem(here + i, spaces)
        return remote(
            buffer.at[peer], buffer.at[peer], send.at[i], recv.at[peer], {"space": peer}
        )

    def each_space(make, act):
        def step(i, carry):
            act(make(i))
            return carry

        lax.fori_loop(1, spaces, step, 0)

    each_space(functools.partial(along_space, stats, send_s, recv_s), lambda c: c.start())

    coeff = (1.0 - 0.05 / members) / (2.0 * members * (members - 1))
    totals[...] = jnp.zeros_like(totals)
    mine.wait()
    aim.wait()

    def score(j, k):
        first, length = cuts[k]
        at = code_ref.at[pl.ds(me * share + first, length)]
        return remote(at, at, send_b.at[j, k], recv_b.at[j, k], {"member": peers[j]})

    for k in range(parts):
        first, length = cuts[k]
        for j in range(3):
            exchange(j, k).wait_recv()

        def channel(c, carry, first=first):
            at = first + c
            f32 = lambda v: v.astype(jnp.float32)
            values = [f32(own[at])] + [f32(arrived[j, at]) for j in range(3)]
            goal = f32(target[at])
            skill = sum(jnp.abs(v - goal) for v in values)
            spread = sum(
                jnp.abs(values[a] - values[b]) for a in range(4) for b in range(a + 1, 4)
            )
            crps = skill / members - coeff * (2.0 * spread)
            code_ref[me * share + at] = encode(crps)
            ocean = (me * share + at >= ATMOS).astype(jnp.float32)
            weight = weights[0] * (1.0 - ocean) + weights[1] * ocean
            totals[pl.ds(at, 1)] = jnp.sum(crps * weight, axis=0, keepdims=True)
            return carry

        lax.fori_loop(0, length, channel, 0, unroll=True)
        for j in range(2):
            score(j, k).start()

    sums[here] = lax.dot_general(
        jnp.ones((8, totals.shape[1]), jnp.float32), totals[...],
        (((1,), (1,)), ((), ())),
        precision=lax.Precision.HIGHEST, preferred_element_type=jnp.float32,
    )
    each_space(functools.partial(along_space, sums, send_t, recv_t), lambda c: c.start())

    each_space(functools.partial(from_space, stats, send_s, recv_s), lambda c: c.wait_recv())

    def add(buffer):
        return lax.fori_loop(
            1, spaces, lambda i, t: t + buffer[i], buffer[0]
        )

    whole = add(stats)
    area = [jnp.sum(whole[g : g + 1], axis=1, keepdims=True) for g in range(2)]
    count = [jnp.sum(whole[2 + g : 3 + g], axis=1, keepdims=True) for g in range(2)]
    scale = [count[g] / area[g] for g in range(2)]
    for g in range(2):
        weight_ref[g] = weights[g] * scale[g]

    def share_sums(j):
        return remote(
            gathered.at[me], gathered.at[me], send_u.at[j], recv_u.at[me], {"member": peers[j]}
        )

    def send_sums():
        each_space(functools.partial(from_space, sums, send_t, recv_t), lambda c: c.wait_recv())
        gathered[me] = add(sums)
        for j in range(3):
            share_sums(j).start()

    def relayed(k):
        return (0, 1) if k % 2 == 0 else (1, 0)

    def arrival(j, k):
        first, length = cuts[k]
        at = code_ref.at[pl.ds(peers[j] * share + first, length)]
        return remote(at, at, send_b.at[j, k], recv_b.at[j, k], {"member": peers[j]})

    def relay(k):
        source, goal = relayed(k)
        first, length = cuts[k]
        at = code_ref.at[pl.ds(peers[source] * share + first, length)]
        return remote(at, at, send_c.at[k], recv_c.at[k], {"member": peers[goal]})

    for k in range(parts):
        arrival(relayed(k)[0], k).wait_recv()
        relay(k).start()
        if k == parts // 2:
            send_sums()

    for j in range(3):
        remote(
            gathered.at[peers[j]], gathered.at[peers[j]], send_u.at[j], recv_u.at[peers[j]],
            {"member": peers[j]},
        ).wait_recv()
    channel_at = (
        lax.broadcasted_iota(jnp.int32, (members, totals.shape[0]), 0) * share
        + lax.broadcasted_iota(jnp.int32, (members, totals.shape[0]), 1)
    )
    rows = jnp.concatenate([gathered[m, 0:1] for m in range(members)], axis=0)
    loss_ref[...] = jnp.where(
        channel_at >= ATMOS, rows * scale[1] / count[1], rows * scale[0] / count[0]
    )
    for k in range(parts):
        arrival(relayed(k)[1], k).wait_recv()
        first, length = cuts[k]
        at = code_ref.at[pl.ds(diagonal * share + first, length)]
        remote(at, at, send_c.at[k], recv_c.at[k], {"member": diagonal}).wait_recv()
    for k in range(parts):
        for j in range(3):
            exchange(j, k).wait_send()
        for j in range(2):
            score(j, k).wait_send()
        relay(k).wait_send()
    each_space(functools.partial(along_space, stats, send_s, recv_s), lambda c: c.wait_send())
    each_space(functools.partial(along_space, sums, send_t, recv_t), lambda c: c.wait_send())
    for j in range(3):
        share_sums(j).wait_send()


def shards(spaces, parts, ensemble_prediction, observed_analysis, validity_flags):
    members = lax.axis_size("member")
    channels, blocks, sites = observed_analysis.shape
    share = channels // members
    dma = pltpu.SemaphoreType.DMA
    wide = -(-share // 128) * 128
    code, weight, loss = pl.pallas_call(
        functools.partial(kernel, members, spaces, share, parts),
        out_shape=(
            jax.ShapeDtypeStruct((channels, blocks, sites), jnp.int16),
            jax.ShapeDtypeStruct((2, blocks, sites), jnp.float32),
            jax.ShapeDtypeStruct((members, wide), jnp.float32),
        ),
        in_specs=[
            pl.BlockSpec(memory_space=pl.ANY),
            pl.BlockSpec(memory_space=pl.ANY),
            pl.BlockSpec(memory_space=pltpu.VMEM),
        ],
        out_specs=(pl.BlockSpec(memory_space=pltpu.VMEM),) * 3,
        scratch_shapes=[
            pltpu.VMEM((share, blocks, sites), jnp.bfloat16),
            pltpu.VMEM((share, blocks, sites), jnp.bfloat16),
            pltpu.VMEM((3, share, blocks, sites), jnp.bfloat16),
            pltpu.VMEM((wide, sites), jnp.float32),
            pltpu.VMEM((spaces, 8, sites), jnp.float32),
            pltpu.VMEM((spaces, 8, wide), jnp.float32),
            pltpu.VMEM((members, 8, wide), jnp.float32),
            dma((2,)),
            dma((3, parts)), dma((3, parts)),
            dma((2, parts)), dma((2, parts)),
            dma((parts,)), dma((parts,)),
            dma((spaces,)), dma((spaces,)),
            dma((spaces,)), dma((spaces,)),
            dma((3,)), dma((members,)),
        ],
        compiler_params=pltpu.CompilerParams(collective_id=0, has_side_effects=True),
    )(ensemble_prediction, observed_analysis, validity_flags)
    is_ocean = jnp.arange(channels, dtype=jnp.int32) >= ATMOS
    weight_chan = jnp.where(is_ocean[:, None, None], weight[1][None], weight[0][None])
    return decode(code) * weight_chan, loss[:, :share].reshape(channels)


def solution(mesh):
    in_specs = (P("member", None, "space", None), P(None, "space", None), P(None, "space", None))
    out_specs = (P(None, "space", None), P())
    return jax.shard_map(
        functools.partial(shards, mesh.shape["space"], 6),
        mesh=mesh, in_specs=in_specs, out_specs=out_specs, check_vma=False,
    )
```

```python
import functools

import jax
import jax.numpy as jnp
from jax import lax
from jax.experimental import pallas as pl
from jax.experimental.pallas import tpu as pltpu
from jax.sharding import PartitionSpec as P

ATMOS = 180
LON = 720
ROWS = 360
MESH = pl.DeviceIdType.MESH

CODES = 1638.0
CENTRE = 16.0
SMALLEST = 2.0**-36
ABSENT = -32768
PLAN = ((1,),(1,),(1,))
INV_LN2 = 1.4426950408889634


def encode(value):
    steps = (jnp.log(jnp.maximum(value, SMALLEST)) * INV_LN2 + CENTRE) * CODES
    code = jnp.floor(steps + 0.5).astype(jnp.int32)
    return jnp.where(value < SMALLEST, ABSENT, code).astype(jnp.int16)


def decode(code):
    code = code.astype(jnp.int32)
    value = jnp.exp2(code.astype(jnp.float32) * (1.0 / CODES) - CENTRE)
    return jnp.where(code == ABSENT, 0.0, value)


def pieces(share, plan):
    flat = [w for group in plan for w in group]
    edges = [share * sum(flat[:i]) // sum(flat) for i in range(len(flat) + 1)]
    cuts = [(a, b - a) for a, b in zip(edges[:-1], edges[1:])]
    groups, at = [], 0
    for group in plan:
        groups.append(range(at, at + len(group)))
        at += len(group)
    return cuts, groups


def kernel(
    members, spaces, share, plan,
    ens_ref, obs_ref, flags_in,
    score_ref, loss_out,
    flags_ref, loss_ref, code_ref, own, target, arrived, totals, stats, sums, gathered,
    local_sem, send_a, recv_a, send_b, recv_b, send_c, recv_c,
    send_s, recv_s, send_t, recv_t, send_u, recv_u,
):
    me = lax.axis_index("member")
    here = lax.axis_index("space")
    x_peer = me + 1 - 2 * lax.rem(me, 2)
    y_peer = lax.rem(me + 2, 4)
    diagonal = 3 - me
    peers = (x_peer, y_peer, diagonal)
    cuts, groups = pieces(share, plan)
    parts = len(cuts)

    def remote(src, dst, send, recv, where):
        return pltpu.make_async_remote_copy(
            src_ref=src, dst_ref=dst, send_sem=send, recv_sem=recv,
            device_id=where, device_id_type=MESH,
        )

    mine = pltpu.make_async_copy(ens_ref.at[0, pl.ds(me * share, share)], own, local_sem.at[0])
    aim = pltpu.make_async_copy(obs_ref.at[pl.ds(me * share, share)], target, local_sem.at[1])
    flags = pltpu.make_async_copy(flags_in, flags_ref, local_sem.at[2])
    loss = pltpu.make_async_copy(loss_ref, loss_out, local_sem.at[3])
    flags.start()
    mine.start()
    aim.start()

    barrier = pltpu.get_barrier_semaphore()
    for peer in peers:
        pl.semaphore_signal(barrier, inc=1, device_id={"member": peer}, device_id_type=MESH)

    def greet(i, carry):
        pl.semaphore_signal(
            barrier, inc=1, device_id={"space": lax.rem(here + i, spaces)}, device_id_type=MESH
        )
        return carry

    lax.fori_loop(1, spaces, greet, 0)
    pl.semaphore_wait(barrier, 3 + spaces - 1)

    def exchange(j, k):
        first = cuts[groups[k][0]][0]
        length = sum(cuts[i][1] for i in groups[k])
        return remote(
            ens_ref.at[0, pl.ds(peers[j] * share + first, length)],
            arrived.at[j, pl.ds(first, length)],
            send_a.at[j, k], recv_a.at[j, k], {"member": peers[j]},
        )

    for k in range(len(groups)):
        for j in (2, 0, 1):
            exchange(j, k).start()

    blocks, sites = flags_ref.shape[1], flags_ref.shape[2]
    lat_rows = min(ROWS, blocks * spaces * sites // LON)
    position = (
        here * (blocks * sites)
        + lax.broadcasted_iota(jnp.int32, (blocks, sites), 0) * sites
        + lax.broadcasted_iota(jnp.int32, (blocks, sites), 1)
    )
    inside = (position < lat_rows * LON).astype(jnp.float32)
    row = jnp.floor((position.astype(jnp.float32) + 0.5) * (1.0 / LON))
    cosine = jnp.cos(jnp.pi * ((row + 0.5) / lat_rows - 0.5))
    flags.wait()
    weights = []
    for g in range(2):
        valid = inside * (flags_ref[g] > 0).astype(jnp.float32)
        weight = cosine * valid
        weights.append(weight)
        for r, part in ((g, weight), (2 + g, valid)):
            stats[here, pl.ds(r, 1)] = jnp.sum(part, axis=0, keepdims=True)

    def along_space(buffer, send, recv, i):
        return remote(
            buffer.at[here], buffer.at[here], send.at[i], recv.at[here],
            {"space": lax.rem(here + i, spaces)},
        )

    def from_space(buffer, send, recv, i):
        peer = lax.rem(here + i, spaces)
        return remote(
            buffer.at[peer], buffer.at[peer], send.at[i], recv.at[peer], {"space": peer}
        )

    def each_space(make, act):
        def step(i, carry):
            act(make(i))
            return carry

        lax.fori_loop(1, spaces, step, 0)

    each_space(functools.partial(along_space, stats, send_s, recv_s), lambda c: c.start())

    coeff = (1.0 - 0.05 / members) / (2.0 * members * (members - 1))
    totals[...] = jnp.zeros_like(totals)
    mine.wait()
    aim.wait()

    def score(j, k):
        first, length = cuts[k]
        at = code_ref.at[pl.ds(me * share + first, length)]
        return remote(at, at, send_b.at[j, k], recv_b.at[j, k], {"member": peers[j]})

    for k in range(parts):
        first, length = cuts[k]
        for i in range(len(groups)):
            if k == groups[i][0]:
                for j in range(3):
                    exchange(j, i).wait_recv()

        def channel(c, carry, first=first):
            at = first + c
            f32 = lambda v: v.astype(jnp.float32)
            values = [f32(own[at])] + [f32(arrived[j, at]) for j in range(3)]
            goal = f32(target[at])
            skill = sum(jnp.abs(v - goal) for v in values)
            spread = sum(
                jnp.abs(values[a] - values[b]) for a in range(4) for b in range(a + 1, 4)
            )
            crps = skill / members - coeff * (2.0 * spread)
            code_ref[me * share + at] = encode(crps)
            ocean = (me * share + at >= ATMOS).astype(jnp.float32)
            weight = weights[0] * (1.0 - ocean) + weights[1] * ocean
            totals[pl.ds(me * share + at, 1)] = jnp.sum(crps * weight, axis=0, keepdims=True)
            return carry

        lax.fori_loop(0, length, channel, 0, unroll=True)
        for j in range(2):
            score(j, k).start()

    sums[here] = lax.dot_general(
        jnp.ones((8, totals.shape[1]), jnp.float32), totals[...],
        (((1,), (1,)), ((), ())),
        precision=lax.Precision.HIGHEST, preferred_element_type=jnp.float32,
    )
    each_space(functools.partial(along_space, sums, send_t, recv_t), lambda c: c.start())

    each_space(functools.partial(from_space, stats, send_s, recv_s), lambda c: c.wait_recv())

    def add(buffer):
        return lax.fori_loop(
            1, spaces, lambda i, t: t + buffer[i], buffer[0]
        )

    whole = add(stats)
    area = [jnp.sum(whole[g : g + 1], axis=1, keepdims=True) for g in range(2)]
    count = [jnp.sum(whole[2 + g : 3 + g], axis=1, keepdims=True) for g in range(2)]
    scale = [count[g] / area[g] for g in range(2)]
    scaled = [weights[g] * scale[g] for g in range(2)]

    def show(owner, k):
        first, length = cuts[k]

        def channel(c, carry):
            at = owner * share + first + c
            ocean = (at >= ATMOS).astype(jnp.float32)
            score_ref[at] = decode(code_ref[at]) * (scaled[0] * (1.0 - ocean) + scaled[1] * ocean)
            return carry

        lax.fori_loop(0, length, channel, 0, unroll=True)

    def share_sums(j):
        return remote(
            gathered.at[me], gathered.at[me], send_u.at[j], recv_u.at[me], {"member": peers[j]}
        )

    def send_sums():
        each_space(functools.partial(from_space, sums, send_t, recv_t), lambda c: c.wait_recv())
        gathered[me] = add(sums)
        for j in range(3):
            share_sums(j).start()

    def relayed(k):
        return (0, 1) if k % 2 == 0 else (1, 0)

    def arrival(j, k):
        first, length = cuts[k]
        at = code_ref.at[pl.ds(peers[j] * share + first, length)]
        return remote(at, at, send_b.at[j, k], recv_b.at[j, k], {"member": peers[j]})

    def relay(k):
        source, goal = relayed(k)
        first, length = cuts[k]
        at = code_ref.at[pl.ds(peers[source] * share + first, length)]
        return remote(at, at, send_c.at[k], recv_c.at[k], {"member": peers[goal]})

    for k in range(parts):
        show(me, k)

    def finish(k):
        first, length = cuts[k]
        at = code_ref.at[pl.ds(diagonal * share + first, length)]
        remote(at, at, send_c.at[k], recv_c.at[k], {"member": diagonal}).wait_recv()
        show(diagonal, k)

    for k in range(parts):
        source, goal = relayed(k)
        arrival(source, k).wait_recv()
        relay(k).start()
        show(peers[source], k)
        if k == parts // 2:
            send_sums()
        arrival(goal, k).wait_recv()
        show(peers[goal], k)
        if k >= 2:
            finish(k - 2)

    for j in range(3):
        remote(
            gathered.at[peers[j]], gathered.at[peers[j]], send_u.at[j], recv_u.at[peers[j]],
            {"member": peers[j]},
        ).wait_recv()
    line = sum(gathered[m] for m in range(members))[0:1]
    channel_at = lax.broadcasted_iota(jnp.int32, line.shape, 1)
    line = jnp.where(channel_at >= ATMOS, line * scale[1] / count[1], line * scale[0] / count[0])
    loss_ref[...] = line.reshape(line.shape[1])[: loss_ref.shape[0]]
    loss.start()
    for k in range(max(parts - 2, 0), parts):
        finish(k)
    for k in range(len(groups)):
        for j in range(3):
            exchange(j, k).wait_send()
    for k in range(parts):
        for j in range(2):
            score(j, k).wait_send()
        relay(k).wait_send()
    each_space(functools.partial(along_space, stats, send_s, recv_s), lambda c: c.wait_send())
    each_space(functools.partial(along_space, sums, send_t, recv_t), lambda c: c.wait_send())
    for j in range(3):
        share_sums(j).wait_send()
    loss.wait()


def shards(spaces, plan, ensemble_prediction, observed_analysis, validity_flags):
    members = lax.axis_size("member")
    channels, blocks, sites = observed_analysis.shape
    share = channels // members
    dma = pltpu.SemaphoreType.DMA
    exchanges, parts = len(plan), sum(len(group) for group in plan)
    wide = -(-channels // 128) * 128
    return pl.pallas_call(
        functools.partial(kernel, members, spaces, share, plan),
        out_shape=(
            pltpu.VMEM((channels, blocks, sites), jnp.float32),
            pltpu.HBM((channels,), jnp.float32),
        ),
        in_specs=[pl.BlockSpec(memory_space=pltpu.HBM)] * 3,
        out_specs=(
            pl.BlockSpec(memory_space=pltpu.VMEM),
            pl.BlockSpec(memory_space=pltpu.HBM),
        ),
        scratch_shapes=[
            pltpu.VMEM(validity_flags.shape, jnp.int32),
            pltpu.VMEM((channels,), jnp.float32),
            pltpu.VMEM((channels, blocks, sites), jnp.int16),
            pltpu.VMEM((share, blocks, sites), jnp.bfloat16),
            pltpu.VMEM((share, blocks, sites), jnp.bfloat16),
            pltpu.VMEM((3, share, blocks, sites), jnp.bfloat16),
            pltpu.VMEM((wide, sites), jnp.float32),
            pltpu.VMEM((spaces, 8, sites), jnp.float32),
            pltpu.VMEM((spaces, 8, wide), jnp.float32),
            pltpu.VMEM((members, 8, wide), jnp.float32),
            dma((4,)),
            dma((3, exchanges)), dma((3, exchanges)),
            dma((2, parts)), dma((2, parts)),
            dma((parts,)), dma((parts,)),
            dma((spaces,)), dma((spaces,)),
            dma((spaces,)), dma((spaces,)),
            dma((3,)), dma((members,)),
        ],
        compiler_params=pltpu.CompilerParams(
            collective_id=0, has_side_effects=True, vmem_limit_bytes=16 * 2**20
        ),
    )(*(
        pltpu.with_memory_space_constraint(v, pltpu.HBM)
        for v in (ensemble_prediction, observed_analysis, validity_flags)
    ))


def solution(mesh):
    in_specs = (P("member", None, "space", None), P(None, "space", None), P(None, "space", None))
    out_specs = (P(None, "space", None), P())
    return jax.shard_map(
        functools.partial(shards, mesh.shape["space"], PLAN),
        mesh=mesh, in_specs=in_specs, out_specs=out_specs, check_vma=False,
    )
```
